128 devices in a mesh: row: 16 (over x, y), col: 8 (over z, core).
Axes of the slice: x: 4, y: 4, z: 4, core: 2. Of those that a mesh axis runs over, the one named last changes fastest.
Arguments:
- activations: bfloat16 [1024, 28672], P('row', 'col'), may hold values from -6 to 6
- act_basis: bfloat16 [28672, 28672], P('col', 'row'), may hold values from -0.03125 to 0.03125
- grads: bfloat16 [1024, 8192], P('col', 'row'), may hold values from -6 to 6
- grad_basis: bfloat16 [8192, 8192], P('row', 'col'), may hold values from -0.0625 to 0.0625
Outputs:
- eigenvalues: float32 [28672, 8192], P('row', 'col')
The draws below stay inside these ranges and needn't reach their ends.
All inputs are finite; a program needn't handle non-finite values.
Results may differ from the reference program's by a relative error of at most 0.0034.
Values may be sent and summed in bfloat16 or wider, within the bound.
A program may use at most 128 MiB of HBM per device.

```python
import math
import jax
import jax.numpy as jnp
from jax import lax

DIN = 28672
DOUT = 8192
SEQS = 4
LEN = 256
TOKENS = 1024


def levels(key, dims, cuts, low, top_value):
    gain = 1.0
    for position, blocks in cuts:
        draws = jax.random.uniform(jax.random.fold_in(jax.random.fold_in(key, 6), position), (blocks,), jnp.float32, low / len(cuts), top_value / len(cuts))
        gain = gain * jnp.repeat(jnp.exp(draws), dims[position] // blocks).reshape((-1,) + (1,) * (len(dims) - 1 - position))
    return gain


def normal_values(key, shape, scale, limit, cuts=(), dtype=jnp.bfloat16):
    gain = levels(key, shape, cuts, -0.22, 0.18) if cuts else 1.0
    result = jax.random.normal(key, shape, jnp.float32) * scale * gain
    return jnp.minimum(jnp.maximum(result, -limit), limit).astype(dtype)


def setup_inputs(seed: int = 0) -> dict:
    key_list = jax.random.split(jax.random.key(seed), 5)
    activations = normal_values(key_list[0], (TOKENS, DIN), 1.0, 6.0, ((0, 16), (1, 8)))
    act_basis = normal_values(key_list[1], (DIN, DIN), DIN ** -0.5, 0.03125, ((0, 8), (1, 16)))
    grads = normal_values(key_list[2], (TOKENS, DOUT), 1.0, 6.0, ((0, 8), (1, 16)))
    grad_basis = normal_values(key_list[3], (DOUT, DOUT), DOUT ** -0.5, 0.0625, ((0, 16), (1, 8)))
    return {"activations": activations, "act_basis": act_basis, "grads": grads, "grad_basis": grad_basis}


def reference(activations, act_basis, grads, grad_basis):
    rotated_acts = jnp.dot(activations, act_basis, preferred_element_type=jnp.float32).astype(jnp.bfloat16)
    rotated_grads = jnp.dot(grads, grad_basis, preferred_element_type=jnp.float32).astype(jnp.bfloat16)
    scale = 1.0 / math.sqrt(LEN)
    total = jnp.zeros((DIN, DOUT), jnp.float32)
    for seq_index in range(SEQS):
        left = rotated_acts[seq_index * LEN:(seq_index + 1) * LEN]
        right = rotated_grads[seq_index * LEN:(seq_index + 1) * LEN]
        products = lax.dot_general(left, right, (((0,), (0,)), ((), ())), preferred_element_type=jnp.float32) * scale
        total = total + products * products
    return total / SEQS
```

```python
import jax
import jax.numpy as jnp
from jax import lax
from jax.experimental import pallas as pl
from jax.experimental.pallas import tpu as pltpu
from jax.sharding import PartitionSpec as P

MESH = pl.DeviceIdType.MESH
BF16, F32 = jnp.bfloat16, jnp.float32
TOKENS, KIN, NIN = 1024, 3584, 1792
KOUT, NOUT = 512, 1024
HALF = NIN // 2
GCOL = NOUT // 2
SEQS, LEN = 4, 256

CHUNKS = (
    ("A00", "A01", "A03", "B00", "B10", "B30"),
    ("A10", "A30", "A02", "B01", "B03", "B20"),
    ("A13", "A33", "A20", "B31", "B33", "B02"),
    ("A11", "A31", "A23", "B11", "B13", "B32"),
    ("A12", "A32", "A21", "A22", "B21", "B23", "B12", "B22"),
)
ROW = {}
for _chunk in CHUNKS:
    for _block in _chunk:
        ROW[_block] = 32 * len(ROW)
BASE = [ROW[chunk[0]] for chunk in CHUNKS]
SIZE = [32 * len(chunk) for chunk in CHUNKS]

RATE = {"x": 1 / 46.6e3, "y": 1 / 46.6e3, "z": 1 / 46.6e3, "d": 1 / 600e3}
DELAY = {"x": 2.2, "y": 2.2, "z": 2.2, "d": 1.0}


def ds(start, size, unit):
    if isinstance(start, int):
        return pl.ds(start, size)
    return pl.ds(pl.multiple_of(start, unit), size)


class Plan:
    def __init__(self):
        self.copies, self.steps = {}, {}
        self.acts()
        self.rotate()
        self.grads()
        self.index = {name: n for n, name in enumerate(self.copies)}

    def copy(self, name, link, nbytes, src, dst):
        self.copies[name] = (link, nbytes, src, dst)

    def step(self, name, rank, waits=(), after=(), cost=0.05, work=None, sends=()):
        self.steps[name] = (rank, tuple(waits), tuple(after), cost, work, tuple(sends))

    def acts(self):
        for half, first, second in (("A", "y", "x"), ("B", "x", "y")):

            def key(u, v, half=half):
                return ROW[half + (f"{v}{u}" if half == "A" else f"{u}{v}")]

            def block(row, low, size):
                return lambda c: c.acts.at[pl.ds(row + low, size), :]

            for r in range(5):
                link = first if r == 0 else second
                u = (0, 0, 3, 1, 2)[r]
                at = (lambda o: key(o, 0)) if r == 0 else (lambda o, u=u: key(u, o))
                for sign, far, low in (("+", 3, 0), ("-", 1, 16)):
                    self.copy(f"{half}d{r}{sign}", link + sign, 32 * KIN * 2, block(at(0), 0, 32), block(at(far), 0, 32))
                    self.copy(f"{half}f{r}{sign}", link + sign, 16 * KIN * 2, block(at(far), low, 16), block(at(2), low, 16))
                    self.step(f"{half}F{r}{sign}", 10 + r, [f"{half}d{r}{sign}"], sends=[f"{half}f{r}{sign}"])
            for r in range(2, 5):
                need = {2: [f"{half}d0+"], 3: [f"{half}d0-"], 4: [f"{half}f0+", f"{half}f0-"]}[r]
                previous = [f"{half}F{r - 2}{s}" for s in "+-"] + [f"{o}F{r - 2}{s}" for s in "+-" for o in "AB"]
                self.step(f"{half}D{r}", 20 + r, need, previous, sends=[f"{half}d{r}+", f"{half}d{r}-"])
        self.step("own", 0, work=lambda c: c.wait_local("acts"), sends=[f"{h}d{r}{s}" for r in (0, 1) for h in "AB" for s in "+-"])

    def ring_sum(self, tag, axis, rank, nbytes, rows, send, recv, add, final, start, sends, gate=()):
        def at(ref, d, h):
            return lambda c: ref(c, rows(c, d, h))

        for name, sign, src, slot in (
            ("a", "+", (2, 1), 0), ("a", "-", (2, 0), 1), ("b", "+", (1, 0), 2),
            ("b", "-", (3, 1), 3), ("c", "+", (1, 1), 4), ("c", "-", (3, 0), 5),
        ):
            self.copy(f"{tag}{name}{sign}", axis + sign, nbytes, at(send, *src), lambda c, slot=slot: recv(c, slot))
        begin = [f"{tag}{n}{s}" for n in "ab" for s in "+-"]
        self.step(f"{tag}S", rank, *start, sends=begin)
        for sign, piece, slot in (("+", (1, 1), 0), ("-", (3, 0), 1)):
            self.step(f"{tag}C{sign}", rank + 1, [f"{tag}a{sign}"], [f"{tag}S"], 0.1,
                      lambda c, piece=piece, slot=slot: add(c, rows(c, *piece), slot), [f"{tag}c{sign}"])
        self.step(f"{tag}E", rank + 2, [f"{tag}{n}{s}" for n in "bc" for s in "+-"], [f"{tag}C+", f"{tag}C-"], 0.2,
                  lambda c: final(c, rows), sends)

    def rotate(self):
        for r in range(5):
            base, size = BASE[r], SIZE[r]
            piece, half = size // 4, size // 8
            offset = base // 8
            need = [f"{h}{n}{s}" for h in "AB" for s in "+-"
                    for n in (("d0",), ("d1", "f0"), ("d2", "f1"), ("d3", "f2"), ("d4", "f3", "f4"))[r]]

            def multiply(c, own, base=base, size=size):
                which = c.k if own else 1 - c.k
                out = c.mine if own else c.other
                if own is False and base == 0:
                    c.wait_local("basis")

                @pl.loop(0, 2)
                def _(n):
                    cols = pl.ds(pl.multiple_of(n * 384, 128), 512)
                    out[pl.ds(base, size), cols] = jnp.dot(
                        c.acts[pl.ds(base, size), :], c.basis[which, :, cols], preferred_element_type=F32)

            cost = 1.8 * size / 192
            before = [] if r == 0 else [f"M{r - 1}m"]
            self.copy(f"{r}core", "d", size * HALF * 4,
                      lambda c, base=base, size=size: c.other.at[pl.ds(base, size), :],
                      lambda c, base=base, size=size: c.partner.at[pl.ds(base, size), :])
            self.step(f"M{r}o", 70 + 2 * r, need, before + ["own"], cost, lambda c, f=multiply: f(c, False), [f"{r}core"])
            self.step(f"M{r}m", 71 + 2 * r, (), [f"M{r}o"], cost, lambda c, f=multiply: f(c, True))

            def rows(c, d, h, base=base, piece=piece, half=half):
                return ds(base + lax.rem(c.z + d, 4) * piece + h * half, half, 8)

            def recv(c, slot, offset=offset, half=half):
                return c.zland.at[slot, pl.ds(offset, half), :]

            def add(c, where, slot, offset=offset, half=half):
                c.mine[where, :] += c.zland[slot, pl.ds(offset, half), :]

            def begin(c, base=base, size=size):
                c.mine[pl.ds(base, size), :] += c.partner[pl.ds(base, size), :]

            def final(c, rows, base=base, piece=piece, half=half, offset=offset):
                parts = []
                for h, one, two in ((0, 2, 5), (1, 3, 4)):
                    parts.append(c.mine[rows(c, 0, h), :] + c.zland[one, pl.ds(offset, half), :] + c.zland[two, pl.ds(offset, half), :])
                whole = jnp.concatenate(parts, axis=0).astype(BF16)
                where = ds(base + c.z * piece, piece, 16)
                for core in range(2):
                    @pl.when(c.k == core)
                    def _(core=core):
                        c.rot[where, pl.ds(core * HALF, HALF)] = whole

            def place(d, low=0, width=HALF, base=base, piece=piece):
                def ref(c):
                    z = lax.rem(c.z + d, 4)
                    return c.rot.at[ds(base + z * piece, piece, 16), pl.ds(pl.multiple_of(c.k * HALF + low, 128), width)]
                return ref

            rank = 40 - 4 * r if False else 40
            nb = piece * HALF * 2
            self.ring_sum(f"{r}z", "z", rank, half * HALF * 4, rows, lambda c, w: c.mine.at[w, :], recv, add, final,
                          ([f"{r}core"], [f"M{r}m"], 0.3, begin), [f"{r}g+", f"{r}g-", f"{r}p0"])
            left = 512 if r % 2 else 384
            self.copy(f"{r}g+", "z+", nb, place(0), place(0))
            self.copy(f"{r}g-", "z-", nb, place(0), place(0))
            self.copy(f"{r}h+", "z+", nb * left // HALF, place(3, 0, left), place(3, 0, left))
            self.copy(f"{r}h-", "z-", nb * (HALF - left) // HALF, place(1, left, HALF - left), place(1, left, HALF - left))
            for n, d in (("p0", 0), ("p1", 1), ("p3", 3), ("p2", 2)):
                self.copy(f"{r}{n}", "d", nb, place(d), place(d))
            self.step(f"{r}H+", 38, [f"{r}g+"], sends=[f"{r}h+", f"{r}p3"])
            self.step(f"{r}H-", 38, [f"{r}g-"], sends=[f"{r}h-", f"{r}p1"])
            self.step(f"{r}L", 39, [f"{r}h+", f"{r}h-"], sends=[f"{r}p2"])

            def store(c, r=r):
                for block in CHUNKS[r]:
                    c.store_acts(block)

            self.step(f"{r}W", 60, [f"{r}p{d}" for d in range(4)], [f"{r}L", f"{r}H+", f"{r}H-"], 0.1, store)

    def grads(self):
        nb = 128 * KOUT * 2

        def shard(d, core, low=0, size=128):
            def ref(c):
                k = c.k if core else 1 - c.k
                return c.grads.at[ds((lax.rem(c.z + d, 4) * 2 + k) * 128 + low, size, 16), :]
            return ref

        self.copy("gz+", "z+", nb, shard(0, 1), shard(0, 1))
        self.copy("gz-", "z-", nb, shard(0, 1), shard(0, 1))
        self.copy("gf+", "z+", nb // 2, shard(3, 1, 0, 64), shard(3, 1, 0, 64))
        self.copy("gf-", "z-", nb // 2, shard(1, 1, 64, 64), shard(1, 1, 64, 64))
        for d in range(4):
            self.copy(f"gp{d}", "d", nb, shard(d, 1), shard(d, 1))
        self.step("G0", 1, after=["own"], work=lambda c: c.wait_local("grads"), sends=["gz+", "gz-", "gp0"])
        self.step("GF+", 2, ["gz+"], ["G0"], sends=["gf+", "gp3"])
        self.step("GF-", 2, ["gz-"], ["G0"], sends=["gf-", "gp1"])
        self.step("GL", 2, ["gf+", "gf-"], ["GF+", "GF-"], sends=["gp2"])

        def multiply(c):
            c.wait_local("gbasis")

            @pl.loop(0, 4)
            def _(n):
                where = pl.ds(pl.multiple_of(n * 256, 256), 256)
                part = jnp.dot(c.grads[where, :], c.gbasis[...], preferred_element_type=F32)
                c.gsum[where, :] = part
                c.gsend[where, :] = part.astype(BF16)

        self.step("GM", 3, [f"gp{d}" for d in range(4)], ["GL"], 2.0, multiply)
        for n, (half, one, two) in enumerate((("A", "x", "y"), ("B", "y", "x"))):
            cols = pl.ds(n * GCOL, GCOL)

            def rows1(c, d, h, one=one):
                return ds(lax.rem(c.pos[one] + d, 4) * 256 + h * 128, 128, 16)

            def add1(c, where, slot, n=n, cols=cols):
                c.gsend[where, cols] = (c.gsum[where, cols] + c.land1[n, slot].astype(F32)).astype(BF16)

            def final1(c, rows, n=n, cols=cols):
                for h, p, q in ((0, 2, 5), (1, 3, 4)):
                    total = c.gsum[rows(c, 0, h), cols] + c.land1[n, p].astype(F32) + c.land1[n, q].astype(F32)
                    c.gsum2[n, pl.ds(h * 128, 128), :] = total
                    c.gsend2[n, pl.ds(h * 128, 128), :] = total.astype(BF16)

            self.ring_sum(f"{half}1", one, 30, 128 * GCOL * 2, rows1, lambda c, w, cols=cols: c.gsend.at[w, cols],
                          lambda c, slot, n=n: c.land1.at[n, slot], add1, final1, ((), ["GM"] + GATE1, 0.05, None), ())

            def rows2(c, d, h, two=two):
                return ds(lax.rem(c.pos[two] + d, 4) * 64 + h * 32, 32, 16)

            def add2(c, where, slot, n=n):
                c.gsend2[n, where, :] = (c.gsum2[n, where, :] + c.land2[n, slot].astype(F32)).astype(BF16)

            def piece(c, d1, d2, one=one, two=two):
                return lax.rem(c.pos[one] + d1, 4) * 256 + lax.rem(c.pos[two] + d2, 4) * 64

            def final2(c, rows, n=n, cols=cols, piece=piece):
                for h, p, q in ((0, 2, 5), (1, 3, 4)):
                    total = c.gsum2[n, rows(c, 0, h), :] + c.land2[n, p].astype(F32) + c.land2[n, q].astype(F32)
                    c.gout[ds(piece(c, 0, 0) + h * 32, 32, 16), cols] = total.astype(BF16)

            def place(d1, d2, low=0, size=64, piece=piece, cols=cols):
                return lambda c: c.gout.at[ds(piece(c, d1, d2) + low, size, 16), cols]

            self.ring_sum(f"{half}2", two, 30, 32 * GCOL * 2, rows2, lambda c, w, n=n: c.gsend2.at[n, w],
                          lambda c, slot, n=n: c.land2.at[n, slot], add2, final2, ((), [f"{half}1E"], 0.05, None),
                          [f"{half}e+", f"{half}e-", f"{half}u0+", f"{half}u0-"])
            nb = 64 * GCOL * 2
            self.copy(f"{half}e+", two + "+", nb, place(0, 0), place(0, 0))
            self.copy(f"{half}e-", two + "-", nb, place(0, 0), place(0, 0))
            self.copy(f"{half}h+", two + "+", nb // 2, place(0, 3, 0, 32), place(0, 3, 0, 32))
            self.copy(f"{half}h-", two + "-", nb // 2, place(0, 1, 32, 32), place(0, 1, 32, 32))
            for j in range(4):
                self.copy(f"{half}u{j}+", one + "+", nb, place(0, j), place(0, j))
                self.copy(f"{half}u{j}-", one + "-", nb, place(0, j), place(0, j))
                self.copy(f"{half}v{j}+", one + "+", nb // 2, place(3, j, 0, 32), place(3, j, 0, 32))
                self.copy(f"{half}v{j}-", one + "-", nb // 2, place(1, j, 32, 32), place(1, j, 32, 32))
                for sign in "+-":
                    self.step(f"{half}V{j}{sign}", 34, [f"{half}u{j}{sign}"], sends=[f"{half}v{j}{sign}"])
            self.step(f"{half}H+", 33, [f"{half}e+"], sends=[f"{half}h+", f"{half}u3+", f"{half}u3-"])
            self.step(f"{half}H-", 33, [f"{half}e-"], sends=[f"{half}h-", f"{half}u1+", f"{half}u1-"])
            self.step(f"{half}L", 33, [f"{half}h+", f"{half}h-"], sends=[f"{half}u2+", f"{half}u2-"])
        every = [f"{h}v{j}{s}" for h in "AB" for j in range(4) for s in "+-"]
        self.step("GW", 80, every, cost=0.1, work=lambda c: c.store_grads())

    def order(self, trace=None):
        now, arrival, free, done, todo, order = 0.0, {}, {}, {}, dict(self.steps), []
        sent_by = {name for spec in self.steps.values() for name in spec[5]}
        assert sent_by == set(self.copies)
        while todo:
            best, soonest = None, None
            for name, (rank, waits, after, cost, _, sends) in todo.items():
                if any(a not in done for a in after) or any(w not in arrival for w in waits):
                    continue
                at = max([arrival[w] for w in waits], default=0.0)
                if at <= now and (best is None or rank < best[0]):
                    best = (rank, name)
                if soonest is None or at < soonest:
                    soonest = at
            if best is None:
                assert soonest is not None, sorted(todo)
                now = soonest
                continue
            name = best[1]
            rank, waits, after, cost, _, sends = todo.pop(name)
            now += cost
            done[name] = now
            order.append(name)
            if trace is not None:
                trace.append((now, name))
            for copy in sends:
                link, nbytes = self.copies[copy][:2]
                free[link] = max(now, free.get(link, 0.0)) + nbytes * RATE[link[0]]
                arrival[copy] = free[link] + DELAY[link[0]]
                if trace is not None:
                    trace.append((arrival[copy], "  arrives " + copy + " " + link))
        return order


GATE1 = ["AD4", "BD4"]


class Context:
    pass


def rotate_kernel(plan, acts_in, basis_in, grads_in, gbasis_in, rot_out, grad_out,
                  acts, basis, mine, other, partner, zland, rot, grads, gbasis, gsum, gsend, gsum2, gsend2, land1, land2, gout,
                  send_sem, recv_sem, load_sem, store_sem):
    c = Context()
    c.acts, c.basis, c.mine, c.other, c.partner, c.zland, c.rot = acts, basis, mine, other, partner, zland, rot
    c.grads, c.gbasis, c.gsum, c.gsend, c.gsum2, c.gsend2 = grads, gbasis, gsum, gsend, gsum2, gsend2
    c.land1, c.land2, c.gout = land1, land2, gout
    row, col = lax.axis_index("row"), lax.axis_index("col")
    c.pos = {"x": row // 4, "y": lax.rem(row, 4)}
    c.z, c.k = col // 2, lax.rem(col, 2)

    def peer(link):
        if link == "d":
            return (row, c.z * 2 + 1 - c.k)
        step = 1 if link[1] == "+" else 3
        if link[0] == "z":
            return (row, lax.rem(c.z + step, 4) * 2 + c.k)
        if link[0] == "x":
            return (lax.rem(c.pos["x"] + step, 4) * 4 + c.pos["y"], col)
        return (c.pos["x"] * 4 + lax.rem(c.pos["y"] + step, 4), col)

    me = col * 128
    loads = {
        "acts": [(acts_in.at[pl.ds(0, 32), :], acts.at[pl.ds(ROW["A00"], 32), :]),
                 (acts_in.at[pl.ds(32, 32), :], acts.at[pl.ds(ROW["B00"], 32), :])],
        "grads": [(grads_in, grads.at[ds(me, 128, 128), :])],
        "gbasis": [(gbasis_in, gbasis)],
        "basis": [(basis_in.at[pl.ds(q * 896, 896), pl.ds(h * HALF, HALF)], basis.at[h, pl.ds(q * 896, 896), :])
                  for q in range(4) for h in range(2)],
    }
    number, local = 0, {}
    for name, pairs in loads.items():
        local[name] = []
        for src, dst in pairs:
            local[name].append(pltpu.make_async_copy(src, dst, load_sem.at[number]))
            number += 1
            local[name][-1].start()

    def wait_local(name):
        for one in local[name]:
            one.wait()

    c.wait_local = wait_local
    stores = []

    def store(src, dst):
        stores.append(pltpu.make_async_copy(src, dst, store_sem.at[len(stores)]))
        stores[-1].start()

    def store_acts(block):
        x, y = lax.rem(c.pos["x"] + int(block[1]), 4), lax.rem(c.pos["y"] + int(block[2]), 4)
        to = (x * 4 + y) * 64 + (0 if block[0] == "A" else 32)
        store(rot.at[pl.ds(ROW[block], 32), :], rot_out.at[ds(to, 32, 32), :])

    c.store_acts = store_acts
    c.store_grads = lambda: store(gout, grad_out)

    barrier = pltpu.get_barrier_semaphore()
    links = ("x+", "x-", "y+", "y-", "z+", "z-", "d")
    for link in links:
        pl.semaphore_signal(barrier, inc=1, device_id=peer(link), device_id_type=MESH)
    pl.semaphore_wait(barrier, len(links))

    started = {}

    def copy_of(name):
        link, _, src, dst = plan.copies[name]
        n = plan.index[name]
        return pltpu.make_async_remote_copy(src_ref=src(c), dst_ref=dst(c), send_sem=send_sem.at[n], recv_sem=recv_sem.at[n],
                                            device_id=peer(link), device_id_type=MESH)

    waited = set()
    for name in plan.order():
        _, waits, _, _, work, sends = plan.steps[name]
        for one in waits:
            if one not in waited:
                waited.add(one)
                started[one].wait_recv()
        if work is not None:
            work(c)
        for one in sends:
            started[one] = copy_of(one)
            started[one].start()
    assert waited == set(plan.copies)
    for one in started.values():
        one.wait_send()
    for one in stores:
        one.wait()


def rotate(activations, act_basis, grads, grad_basis):
    plan = Plan()
    count = len(plan.copies)
    anywhere = pl.BlockSpec(memory_space=pl.ANY)
    return pl.pallas_call(
        lambda *refs: rotate_kernel(plan, *refs),
        out_shape=[jax.ShapeDtypeStruct((TOKENS, NIN), BF16), jax.ShapeDtypeStruct((TOKENS, NOUT), BF16)],
        in_specs=[anywhere] * 4,
        out_specs=[anywhere] * 2,
        scratch_shapes=[
            pltpu.VMEM((TOKENS, KIN), BF16),
            pltpu.VMEM((2, KIN, HALF), BF16),
            pltpu.VMEM((TOKENS, HALF), F32),
            pltpu.VMEM((TOKENS, HALF), F32),
            pltpu.VMEM((TOKENS, HALF), F32),
            pltpu.VMEM((6, TOKENS // 8, HALF), F32),
            pltpu.VMEM((TOKENS, NIN), BF16),
            pltpu.VMEM((TOKENS, KOUT), BF16),
            pltpu.VMEM((KOUT, NOUT), BF16),
            pltpu.VMEM((TOKENS, NOUT), F32),
            pltpu.VMEM((TOKENS, NOUT), BF16),
            pltpu.VMEM((2, 256, GCOL), F32),
            pltpu.VMEM((2, 256, GCOL), BF16),
            pltpu.VMEM((2, 6, 128, GCOL), BF16),
            pltpu.VMEM((2, 6, 32, GCOL), BF16),
            pltpu.VMEM((TOKENS, NOUT), BF16),
            pltpu.SemaphoreType.DMA((count,)),
            pltpu.SemaphoreType.DMA((count,)),
            pltpu.SemaphoreType.DMA((12,)),
            pltpu.SemaphoreType.DMA((33,)),
        ],
        compiler_params=pltpu.CompilerParams(collective_id=0, has_side_effects=True, vmem_limit_bytes=60 * 2**20),
        name="rotate",
    )(activations, act_basis, grads, grad_basis)


def square_kernel(rot, grad, out):
    total = None
    for s in range(SEQS):
        where = pl.ds(s * LEN, LEN)
        products = lax.dot_general(rot[where, :], grad[where, :], (((0,), (0,)), ((), ())), preferred_element_type=F32)
        total = products * products if total is None else total + products * products
    out[...] = total * (1.0 / (LEN * SEQS))


def square(rot, grad):
    rows = 256
    return pl.pallas_call(
        square_kernel,
        out_shape=jax.ShapeDtypeStruct((NIN, NOUT), F32),
        grid=(NIN // rows,),
        in_specs=[pl.BlockSpec((TOKENS, rows), lambda i: (0, i)), pl.BlockSpec((TOKENS, NOUT), lambda i: (0, 0))],
        out_specs=pl.BlockSpec((rows, NOUT), lambda i: (i, 0)),
        compiler_params=pltpu.CompilerParams(dimension_semantics=("arbitrary",)),
        name="square",
    )(rot, grad)


def shards(activations, act_basis, grads, grad_basis):
    return square(*rotate(activations, act_basis, grads, grad_basis))


def solution(mesh):
    return jax.shard_map(
        shards,
        mesh=mesh,
        in_specs=(P("row", "col"), P("col", "row"), P("col", "row"), P("row", "col")),
        out_specs=P("row", "col"),
        check_vma=False,
    )
```

```python
import jax
import jax.numpy as jnp
from jax import lax
from jax.experimental import pallas as pl
from jax.experimental.pallas import tpu as pltpu
from jax.sharding import PartitionSpec as P

MESH = pl.DeviceIdType.MESH
BF16, F32 = jnp.bfloat16, jnp.float32
TOKENS, KIN, NIN = 1024, 3584, 1792
KOUT, NOUT = 512, 1024
HALF = NIN // 2
GCOL = NOUT // 2
SEQS, LEN = 4, 256
PARTS = ((0, 512), (512, 384))

CHUNKS = (
    ("A00", "A01", "A03", "B00", "B10", "B30"),
    ("A10", "A30", "A02", "B01", "B03", "B20"),
    ("A13", "A33", "A20", "B31", "B33", "B02"),
    ("A11", "A31", "A23", "B11", "B13", "B32"),
    ("A12", "A32", "A21", "B21", "B23", "B12"),
    ("A22", "B22"),
)
ROW = {}
for _chunk in CHUNKS:
    for _block in _chunk:
        ROW[_block] = 32 * len(ROW)
BASE = [ROW[chunk[0]] for chunk in CHUNKS]
SIZE = [32 * len(chunk) for chunk in CHUNKS]


def ds(start, size, unit):
    if isinstance(start, int):
        return pl.ds(start, size)
    return pl.ds(pl.multiple_of(start, unit), size)


class Plan:
    def __init__(self):
        self.copies, self.steps = {}, {}
        self.acts()
        self.rotate()
        self.grads()
        self.index = {name: n for n, name in enumerate(self.copies)}

    def copy(self, name, link, nbytes, src, dst):
        self.copies[name] = (link, nbytes, src, dst)

    def step(self, name, rank, waits=(), after=(), cost=0.05, work=None, sends=()):
        self.steps[name] = (rank, tuple(waits), tuple(after), cost, work, tuple(sends))

    def acts(self):
        for half, first, second in (("A", "y", "x"), ("B", "x", "y")):

            def key(u, v, half=half):
                return ROW[half + (f"{v}{u}" if half == "A" else f"{u}{v}")]

            def block(row, low, size):
                return lambda c: c.acts.at[pl.ds(row + low, size), :]

            for r in range(5):
                link = first if r == 0 else second
                u = (0, 0, 3, 1, 2)[r]
                at = (lambda o: key(o, 0)) if r == 0 else (lambda o, u=u: key(u, o))
                for sign, far, low in (("+", 3, 0), ("-", 1, 16)):
                    self.copy(f"{half}d{r}{sign}", link + sign, 32 * KIN * 2, block(at(0), 0, 32), block(at(far), 0, 32))
                    self.copy(f"{half}f{r}{sign}", link + sign, 16 * KIN * 2, block(at(far), low, 16), block(at(2), low, 16))
                    self.step(f"{half}F{r}{sign}", 10 + r, [f"{half}d{r}{sign}"], sends=[f"{half}f{r}{sign}"])
            for r in range(2, 5):
                need = {2: [f"{half}d0+"], 3: [f"{half}d0-"], 4: [f"{half}f0+", f"{half}f0-"]}[r]
                previous = [f"{half}F{r - 2}{s}" for s in "+-"] + [f"{o}F{r - 2}{s}" for s in "+-" for o in "AB"]
                self.step(f"{half}D{r}", 20 + r, need, previous, sends=[f"{half}d{r}+", f"{half}d{r}-"])
        self.step("own", 0, work=lambda c: c.wait_local("acts"), sends=[f"{h}d{r}{s}" for r in (0, 1) for h in "AB" for s in "+-"])

    def ring_sum(self, tag, axis, rank, nbytes, rows, send, recv, add, final, start, sends, gate=()):
        def at(ref, d, h):
            return lambda c: ref(c, rows(c, d, h))

        for name, sign, src, slot in (
            ("a", "+", (2, 1), 0), ("a", "-", (2, 0), 1), ("b", "+", (1, 0), 2),
            ("b", "-", (3, 1), 3), ("c", "+", (1, 1), 4), ("c", "-", (3, 0), 5),
        ):
            self.copy(f"{tag}{name}{sign}", axis + sign, nbytes, at(send, *src), lambda c, slot=slot: recv(c, slot))
        begin = [f"{tag}{n}{s}" for n in "ab" for s in "+-"]
        self.step(f"{tag}S", rank, *start, sends=begin)
        for sign, piece, slot in (("+", (1, 1), 0), ("-", (3, 0), 1)):
            self.step(f"{tag}C{sign}", rank + 1, [f"{tag}a{sign}"], [f"{tag}S"], 0.1,
                      lambda c, piece=piece, slot=slot: add(c, rows(c, *piece), slot), [f"{tag}c{sign}"])
        self.step(f"{tag}E", rank + 2, [f"{tag}{n}{s}" for n in "bc" for s in "+-"], [f"{tag}C+", f"{tag}C-"], 0.2,
                  lambda c: final(c, rows), sends)

    def rotate(self):
        for r in range(6):
            base, size = BASE[r], SIZE[r]
            piece, half = size // 4, size // 8
            offset = base // 8
            need = [f"{h}{n}{s}" for h in "AB" for s in "+-"
                    for n in (("d0",), ("d1", "f0"), ("d2", "f1"), ("d3", "f2"), ("d4", "f3"), ("f4",))[r]]

            def multiply(c, own, cols, base=base, size=size):
                which = c.k if own else 1 - c.k
                out = c.mine if own else c.other
                if not own and base == 0 and cols == PARTS[0]:
                    c.wait_local("basis")
                where, cols = pl.ds(base, size), pl.ds(*cols)
                out[where, cols] = jnp.dot(c.acts[where, :], c.basis[which, :, cols], preferred_element_type=F32)

            cost = {192: 0.88, 64: 0.62}[size]
            last = f"M{r - 1}m1" if r else "own"
            for own in (False, True):
                for n, cols in enumerate(PARTS):
                    name = f"M{r}{'m' if own else 'o'}{n}"
                    sends = []
                    if not own:
                        sends = [f"{r}core{n}"]
                        self.copy(sends[0], "d", size * cols[1] * 4,
                                  lambda c, base=base, size=size, cols=cols: c.other.at[pl.ds(base, size), pl.ds(*cols)],
                                  lambda c, base=base, size=size, cols=cols: c.partner.at[pl.ds(base, size), pl.ds(*cols)])
                    self.step(name, 70 + 4 * r + 2 * own + n, () if own or n else need, [last], cost,
                              lambda c, f=multiply, own=own, cols=cols: f(c, own, cols), sends)
                    last = name

            def rows(c, d, h, base=base, piece=piece, half=half):
                return ds(base + lax.rem(c.z + d, 4) * piece + h * half, half, 8)

            def recv(c, slot, offset=offset, half=half):
                return c.zland.at[slot, pl.ds(offset, half), :]

            def add(c, where, slot, offset=offset, half=half):
                c.mine[where, :] += c.zland[slot, pl.ds(offset, half), :]

            def begin(c, base=base, size=size):
                c.mine[pl.ds(base, size), :] += c.partner[pl.ds(base, size), :]

            def final(c, rows, base=base, piece=piece, half=half, offset=offset):
                parts = []
                for h, one, two in ((0, 2, 5), (1, 3, 4)):
                    parts.append(c.mine[rows(c, 0, h), :] + c.zland[one, pl.ds(offset, half), :] + c.zland[two, pl.ds(offset, half), :])
                whole = jnp.concatenate(parts, axis=0).astype(BF16)
                where = ds(base + c.z * piece, piece, 16)
                for core in range(2):
                    @pl.when(c.k == core)
                    def _(core=core):
                        c.rot[where, pl.ds(core * HALF, HALF)] = whole

            def place(d, low=0, width=HALF, base=base, piece=piece):
                def ref(c):
                    z = lax.rem(c.z + d, 4)
                    return c.rot.at[ds(base + z * piece, piece, 16), pl.ds(pl.multiple_of(c.k * HALF + low, 128), width)]
                return ref

            rank = 40
            nb = piece * HALF * 2
            self.ring_sum(f"{r}z", "z", rank, half * HALF * 4, rows, lambda c, w: c.mine.at[w, :], recv, add, final,
                          ([f"{r}core0", f"{r}core1"], [f"M{r}m1"], 0.3, begin), [f"{r}g+", f"{r}g-", f"{r}p0"])
            left = 512 if r % 2 else 384
            self.copy(f"{r}g+", "z+", nb, place(0), place(0))
            self.copy(f"{r}g-", "z-", nb, place(0), place(0))
            self.copy(f"{r}h+", "z+", nb * left // HALF, place(3, 0, left), place(3, 0, left))
            self.copy(f"{r}h-", "z-", nb * (HALF - left) // HALF, place(1, left, HALF - left), place(1, left, HALF - left))
            for n, d in (("p0", 0), ("p1", 1), ("p3", 3), ("p2", 2)):
                self.copy(f"{r}{n}", "d", nb, place(d), place(d))
            self.step(f"{r}H+", 38, [f"{r}g+"], sends=[f"{r}h+", f"{r}p3"])
            self.step(f"{r}H-", 38, [f"{r}g-"], sends=[f"{r}h-", f"{r}p1"])
            self.step(f"{r}L", 39, [f"{r}h+", f"{r}h-"], sends=[f"{r}p2"])

            self.step(f"{r}W", 90, [f"{r}p{d}" for d in range(4)], [f"{r}L", f"{r}H+", f"{r}H-"])

    def grads(self):
        nb = 128 * KOUT * 2

        def shard(d, core, low=0, size=128):
            def ref(c):
                k = c.k if core else 1 - c.k
                return c.grads.at[ds((lax.rem(c.z + d, 4) * 2 + k) * 128 + low, size, 16), :]
            return ref

        self.copy("gz+", "z+", nb, shard(0, 1), shard(0, 1))
        self.copy("gz-", "z-", nb, shard(0, 1), shard(0, 1))
        self.copy("gf+", "z+", nb // 2, shard(3, 1, 0, 64), shard(3, 1, 0, 64))
        self.copy("gf-", "z-", nb // 2, shard(1, 1, 64, 64), shard(1, 1, 64, 64))
        for d in range(4):
            self.copy(f"gp{d}", "d", nb, shard(d, 1), shard(d, 1))
        self.step("G0", 1, after=["own"], work=lambda c: c.wait_local("grads"), sends=["gz+", "gz-", "gp0"])
        self.step("GF+", 2, ["gz+"], ["G0"], sends=["gf+", "gp3"])
        self.step("GF-", 2, ["gz-"], ["G0"], sends=["gf-", "gp1"])
        self.step("GL", 2, ["gf+", "gf-"], ["GF+", "GF-"], sends=["gp2"])

        def multiply(c):
            c.wait_local("gbasis")

            @pl.loop(0, 4)
            def _(n):
                where = pl.ds(pl.multiple_of(n * 256, 256), 256)
                part = jnp.dot(c.grads[where, :], c.gbasis[...], preferred_element_type=F32)
                c.gsum[where, :] = part
                c.gsend[where, :] = part.astype(BF16)

        self.step("GM", 3, [f"gp{d}" for d in range(4)], ["GL"], 2.0, multiply)
        for n, (half, one, two) in enumerate((("A", "x", "y"), ("B", "y", "x"))):
            cols = pl.ds(n * GCOL, GCOL)

            def rows1(c, d, h, one=one):
                return ds(lax.rem(c.pos[one] + d, 4) * 256 + h * 128, 128, 16)

            def add1(c, where, slot, n=n, cols=cols):
                c.gsend[where, cols] = (c.gsum[where, cols] + c.land1[n, slot].astype(F32)).astype(BF16)

            def final1(c, rows, n=n, cols=cols):
                for h, p, q in ((0, 2, 5), (1, 3, 4)):
                    total = c.gsum[rows(c, 0, h), cols] + c.land1[n, p].astype(F32) + c.land1[n, q].astype(F32)
                    c.gsum2[n, pl.ds(h * 128, 128), :] = total
                    c.gsend2[n, pl.ds(h * 128, 128), :] = total.astype(BF16)

            self.ring_sum(f"{half}1", one, 30, 128 * GCOL * 2, rows1, lambda c, w, cols=cols: c.gsend.at[w, cols],
                          lambda c, slot, n=n: c.land1.at[n, slot], add1, final1, ((), ["GM"], 0.05, None), ())

            def rows2(c, d, h, two=two):
                return ds(lax.rem(c.pos[two] + d, 4) * 64 + h * 32, 32, 16)

            def add2(c, where, slot, n=n):
                c.gsend2[n, where, :] = (c.gsum2[n, where, :] + c.land2[n, slot].astype(F32)).astype(BF16)

            def piece(c, d1, d2, one=one, two=two):
                return lax.rem(c.pos[one] + d1, 4) * 256 + lax.rem(c.pos[two] + d2, 4) * 64

            def final2(c, rows, n=n, cols=cols, piece=piece):
                for h, p, q in ((0, 2, 5), (1, 3, 4)):
                    total = c.gsum2[n, rows(c, 0, h), :] + c.land2[n, p].astype(F32) + c.land2[n, q].astype(F32)
                    c.gout[ds(piece(c, 0, 0) + h * 32, 32, 16), cols] = total.astype(BF16)

            def place(d1, d2, low=0, size=64, piece=piece, cols=cols):
                return lambda c: c.gout.at[ds(piece(c, d1, d2) + low, size, 16), cols]

            self.ring_sum(f"{half}2", two, 30, 32 * GCOL * 2, rows2, lambda c, w, n=n: c.gsend2.at[n, w],
                          lambda c, slot, n=n: c.land2.at[n, slot], add2, final2, ((), [f"{half}1E"], 0.05, None),
                          [f"{half}e+", f"{half}e-", f"{half}u0+", f"{half}u0-"])
            nb = 64 * GCOL * 2
            self.copy(f"{half}e+", two + "+", nb, place(0, 0), place(0, 0))
            self.copy(f"{half}e-", two + "-", nb, place(0, 0), place(0, 0))
            self.copy(f"{half}h+", two + "+", nb // 2, place(0, 3, 0, 32), place(0, 3, 0, 32))
            self.copy(f"{half}h-", two + "-", nb // 2, place(0, 1, 32, 32), place(0, 1, 32, 32))
            for j in range(4):
                self.copy(f"{half}u{j}+", one + "+", nb, place(0, j), place(0, j))
                self.copy(f"{half}u{j}-", one + "-", nb, place(0, j), place(0, j))
                self.copy(f"{half}v{j}+", one + "+", nb // 2, place(3, j, 0, 32), place(3, j, 0, 32))
                self.copy(f"{half}v{j}-", one + "-", nb // 2, place(1, j, 32, 32), place(1, j, 32, 32))
                for sign in "+-":
                    self.step(f"{half}V{j}{sign}", 34, [f"{half}u{j}{sign}"], sends=[f"{half}v{j}{sign}"])
            self.step(f"{half}H+", 33, [f"{half}e+"], sends=[f"{half}h+", f"{half}u3+", f"{half}u3-"])
            self.step(f"{half}H-", 33, [f"{half}e-"], sends=[f"{half}h-", f"{half}u1+", f"{half}u1-"])
            self.step(f"{half}L", 33, [f"{half}h+", f"{half}h-"], sends=[f"{half}u2+", f"{half}u2-"])
        every = [f"{h}v{j}{s}" for h in "AB" for j in range(4) for s in "+-"]
        self.step("GW", 90, every)


ORDER = (
    "own", "G0", "M0o0", "AF0+", "M0o1", "GF-", "BF0-", "AF0-", "BF0+", "AD2", "BD2", "GF+", "BF1-", "M0m0", "AF1+", "M0m1",
    "M1o0", "0zS", "AF1-", "BF1+", "M1o1", "M1m0", "AD3", "GL", "M1m1", "BD3", "1zS", "GM", "0zC-", "AF2+", "AF2-", "BF2+",
    "M2o0", "0zC+", "BF2-", "M2o1", "M2m0", "A1S", "1zC-", "AD4", "B1S", "1zC+", "M2m1", "BD4", "2zS", "0zE", "M3o0", "M3o1",
    "M3m0", "2zC+", "2zC-", "M3m1", "A1C-", "A1C+", "3zS", "B1C+", "B1C-", "1zE", "3zC+", "3zC-", "AF3+", "BF3-", "BF3+",
    "AF3-", "1H-", "B1E", "BF4+", "0H-", "B2S", "BF4-", "2zE", "A1E", "0H+", "AF4+", "AF4-", "A2S", "3zE", "1H+", "M4o0",
    "M4o1", "B2C+", "B2C-", "M4m0", "M4m1", "4zS", "A2C+", "A2C-", "M5o0", "B2E", "M5o1", "M5m0", "M5m1", "0L", "5zS", "A2E",
    "4zC+", "4zC-", "BH-", "BH+", "5zC-", "2H-", "5zC+", "AH+", "2H+", "AH-", "BL", "4zE", "5zE", "BV1-", "3H+", "BV1+",
    "1L", "AV0-", "BV0-", "3H-", "AL", "BV0+", "BV3+", "AV0+", "0W", "AV3-", "BV3-", "BV2-", "BV2+", "AV1+", "AV3+", "AV1-",
    "4H-", "4H+", "5H+", "5H-", "AV2+", "AV2-", "3L", "2L", "3W", "4L", "2W", "5L", "1W", "4W", "GW", "5W",
)


class Context:
    pass


def rotate_kernel(plan, acts_in, basis_in, grads_in, gbasis_in, rot, gout,
                  acts, basis, mine, other, partner, zland, grads, gbasis, gsum, gsend, gsum2, gsend2, land1, land2,
                  send_sem, recv_sem, load_sem):
    c = Context()
    c.acts, c.basis, c.mine, c.other, c.partner, c.zland, c.rot = acts, basis, mine, other, partner, zland, rot
    c.grads, c.gbasis, c.gsum, c.gsend, c.gsum2, c.gsend2 = grads, gbasis, gsum, gsend, gsum2, gsend2
    c.land1, c.land2, c.gout = land1, land2, gout
    row, col = lax.axis_index("row"), lax.axis_index("col")
    c.pos = {"x": row // 4, "y": lax.rem(row, 4)}
    c.z, c.k = col // 2, lax.rem(col, 2)

    def peer(link):
        if link == "d":
            return (row, c.z * 2 + 1 - c.k)
        step = 1 if link[1] == "+" else 3
        if link[0] == "z":
            return (row, lax.rem(c.z + step, 4) * 2 + c.k)
        if link[0] == "x":
            return (lax.rem(c.pos["x"] + step, 4) * 4 + c.pos["y"], col)
        return (c.pos["x"] * 4 + lax.rem(c.pos["y"] + step, 4), col)

    me = col * 128
    loads = {
        "acts": [(acts_in.at[pl.ds(0, 32), :], acts.at[pl.ds(ROW["A00"], 32), :]),
                 (acts_in.at[pl.ds(32, 32), :], acts.at[pl.ds(ROW["B00"], 32), :])],
        "grads": [(grads_in, grads.at[ds(me, 128, 128), :])],
        "gbasis": [(gbasis_in, gbasis)],
        "basis": [(basis_in.at[pl.ds(q * 896, 896), pl.ds(h * HALF, HALF)], basis.at[h, pl.ds(q * 896, 896), :])
                  for q in range(4) for h in range(2)],
    }
    number, local = 0, {}
    for name, pairs in loads.items():
        local[name] = []
        for src, dst in pairs:
            local[name].append(pltpu.make_async_copy(src, dst, load_sem.at[number]))
            number += 1
            local[name][-1].start()

    def wait_local(name):
        for one in local[name]:
            one.wait()

    c.wait_local = wait_local
    barrier = pltpu.get_barrier_semaphore()
    links = ("x+", "x-", "y+", "y-", "z+", "z-", "d")
    for link in links:
        pl.semaphore_signal(barrier, inc=1, device_id=peer(link), device_id_type=MESH)
    pl.semaphore_wait(barrier, len(links))

    started = {}

    def copy_of(name):
        link, _, src, dst = plan.copies[name]
        n = plan.index[name]
        return pltpu.make_async_remote_copy(src_ref=src(c), dst_ref=dst(c), send_sem=send_sem.at[n], recv_sem=recv_sem.at[n],
                                            device_id=peer(link), device_id_type=MESH)

    waited = set()
    for name in ORDER:
        _, waits, _, _, work, sends = plan.steps[name]
        for one in waits:
            if one not in waited:
                waited.add(one)
                started[one].wait_recv()
        if work is not None:
            work(c)
        for one in sends:
            started[one] = copy_of(one)
            started[one].start()
    assert waited == set(plan.copies)
    for one in started.values():
        one.wait_send()


def rotate(activations, act_basis, grads, grad_basis):
    plan = Plan()
    count = len(plan.copies)
    anywhere = pl.BlockSpec(memory_space=pl.ANY)
    return pl.pallas_call(
        lambda *refs: rotate_kernel(plan, *refs),
        out_shape=[pltpu.VMEM((TOKENS, NIN), BF16), pltpu.VMEM((TOKENS, NOUT), BF16)],
        in_specs=[anywhere] * 4,
        out_specs=[pl.BlockSpec(memory_space=pltpu.VMEM)] * 2,
        scratch_shapes=[
            pltpu.VMEM((TOKENS, KIN), BF16),
            pltpu.VMEM((2, KIN, HALF), BF16),
            pltpu.VMEM((TOKENS, HALF), F32),
            pltpu.VMEM((TOKENS, HALF), F32),
            pltpu.VMEM((TOKENS, HALF), F32),
            pltpu.VMEM((6, TOKENS // 8, HALF), F32),
            pltpu.VMEM((TOKENS, KOUT), BF16),
            pltpu.VMEM((KOUT, NOUT), BF16),
            pltpu.VMEM((TOKENS, NOUT), F32),
            pltpu.VMEM((TOKENS, NOUT), BF16),
            pltpu.VMEM((2, 256, GCOL), F32),
            pltpu.VMEM((2, 256, GCOL), BF16),
            pltpu.VMEM((2, 6, 128, GCOL), BF16),
            pltpu.VMEM((2, 6, 32, GCOL), BF16),
            pltpu.SemaphoreType.DMA((count,)),
            pltpu.SemaphoreType.DMA((count,)),
            pltpu.SemaphoreType.DMA((12,)),
        ],
        compiler_params=pltpu.CompilerParams(collective_id=0, has_side_effects=True, vmem_limit_bytes=50 * 2**20),
        name="rotate",
    )(activations, act_basis, grads, grad_basis)


def square_kernel(rot, grad, out):
    row = lax.axis_index("row")
    x, y = row // 4, lax.rem(row, 4)
    total = None
    for i in range(4):
        blocks = [(half, i, j) for half in "AB" for j in range(4)]
        left = jnp.concatenate([rot[pl.ds(ROW[f"{h}{i}{j}"], 32), :] for h, i, j in blocks], axis=0)
        right = []
        for h, i, j in blocks:
            token = (lax.rem(x + i, 4) * 4 + lax.rem(y + j, 4)) * 64 + (0 if h == "A" else 32)
            right.append(grad[ds(token, 32, 32), :])
        right = jnp.concatenate(right, axis=0)
        products = lax.dot_general(left, right, (((0,), (0,)), ((), ())), preferred_element_type=F32)
        total = products * products if total is None else total + products * products
    out[...] = total * (1.0 / (LEN * SEQS))


def square(rot, grad):
    rows = 256
    return pl.pallas_call(
        square_kernel,
        out_shape=jax.ShapeDtypeStruct((NIN, NOUT), F32),
        grid=(NIN // rows,),
        in_specs=[pl.BlockSpec((TOKENS, rows), lambda i: (0, i)), pl.BlockSpec((TOKENS, NOUT), lambda i: (0, 0))],
        out_specs=pl.BlockSpec((rows, NOUT), lambda i: (i, 0)),
        compiler_params=pltpu.CompilerParams(dimension_semantics=("arbitrary",), vmem_limit_bytes=20 * 2**20),
        name="square",
    )(rot, grad)


def shards(activations, act_basis, grads, grad_basis):
    return square(*rotate(activations, act_basis, grads, grad_basis))


def solution(mesh):
    return jax.shard_map(
        shards,
        mesh=mesh,
        in_specs=(P("row", "col"), P("col", "row"), P("col", "row"), P("row", "col")),
        out_specs=P("row", "col"),
        check_vma=False,
    )
```

```python
import jax
import jax.numpy as jnp
from jax import lax
from jax.experimental import pallas as pl
from jax.experimental.pallas import tpu as pltpu
from jax.sharding import PartitionSpec as P

MESH = pl.DeviceIdType.MESH
BF16, F32 = jnp.bfloat16, jnp.float32
TOKENS, KIN, NIN = 1024, 3584, 1792
KOUT, NOUT = 512, 1024
HALF = NIN // 2
GCOL = NOUT // 4
SEQS, LEN = 4, 256
PARTS = ((0, 512), (512, 384))

CHUNKS = (
    ("A00", "A01", "A03", "B00", "B10", "B30"),
    ("A10", "A30", "A02", "B01", "B03", "B20"),
    ("A13", "A33", "A20", "B31", "B33", "B02"),
    ("A11", "A31", "A23", "B11", "B13", "B32"),
    ("A12", "A32", "A21", "B21", "B23", "B12"),
    ("A22", "B22"),
)
ROW = {}
for _chunk in CHUNKS:
    for _block in _chunk:
        ROW[_block] = 32 * len(ROW)
BASE = [ROW[chunk[0]] for chunk in CHUNKS]
SIZE = [32 * len(chunk) for chunk in CHUNKS]

def ds(start, size, unit):
    if isinstance(start, int):
        return pl.ds(start, size)
    return pl.ds(pl.multiple_of(start, unit), size)


class Plan:
    def __init__(self):
        self.copies, self.steps = {}, {}
        self.acts()
        self.rotate()
        self.grads()
        self.index = {name: n for n, name in enumerate(self.copies)}

    def copy(self, name, link, nbytes, src, dst):
        self.copies[name] = (link, nbytes, src, dst)

    def step(self, name, rank, waits=(), after=(), cost=0.05, work=None, sends=()):
        self.steps[name] = (rank, tuple(waits), tuple(after), cost, work, tuple(sends))

    def acts(self):
        for half, first, second in (("A", "y", "x"), ("B", "x", "y")):

            def key(u, v, half=half):
                return ROW[half + (f"{v}{u}" if half == "A" else f"{u}{v}")]

            def block(row, low, size):
                return lambda c: c.acts.at[pl.ds(row + low, size), :]

            for r in range(5):
                link = first if r == 0 else second
                u = (0, 0, 3, 1, 2)[r]
                at = (lambda o: key(o, 0)) if r == 0 else (lambda o, u=u: key(u, o))
                for sign, far, low in (("+", 3, 0), ("-", 1, 16)):
                    self.copy(f"{half}d{r}{sign}", link + sign, 32 * KIN * 2, block(at(0), 0, 32), block(at(far), 0, 32))
                    self.copy(f"{half}f{r}{sign}", link + sign, 16 * KIN * 2, block(at(far), low, 16), block(at(2), low, 16))
                    self.step(f"{half}F{r}{sign}", 10 + r, [f"{half}d{r}{sign}"], sends=[f"{half}f{r}{sign}"])
            for r in range(2, 5):
                need = {2: [f"{half}d0+"], 3: [f"{half}d0-"], 4: [f"{half}f0+", f"{half}f0-"]}[r]
                previous = [f"{half}F{r - 2}{s}" for s in "+-"] + [f"{o}F{r - 2}{s}" for s in "+-" for o in "AB"]
                self.step(f"{half}D{r}", 20 + r, need, previous, sends=[f"{half}d{r}+", f"{half}d{r}-"])
        self.step("own", 0, work=lambda c: c.wait_local("acts"), sends=[f"{h}d{r}{s}" for r in (0, 1) for h in "AB" for s in "+-"])

    def ring_sum(self, tag, axis, rank, nbytes, rows, send, recv, add, final, start, sends, gate=()):
        def at(ref, d, h):
            return lambda c: ref(c, rows(c, d, h))

        for name, sign, src, slot in (
            ("a", "+", (2, 1), 0), ("a", "-", (2, 0), 1), ("b", "+", (1, 0), 2),
            ("b", "-", (3, 1), 3), ("c", "+", (1, 1), 4), ("c", "-", (3, 0), 5),
        ):
            self.copy(f"{tag}{name}{sign}", axis + sign, nbytes, at(send, *src), lambda c, slot=slot: recv(c, slot))
        begin = [f"{tag}{n}{s}" for n in "ab" for s in "+-"]
        self.step(f"{tag}S", rank, *start, sends=begin)
        for sign, piece, slot in (("+", (1, 1), 0), ("-", (3, 0), 1)):
            self.step(f"{tag}C{sign}", rank + 1, [f"{tag}a{sign}"], [f"{tag}S"], 0.1,
                      lambda c, piece=piece, slot=slot: add(c, rows(c, *piece), slot), [f"{tag}c{sign}"])
        self.step(f"{tag}E", rank + 2, [f"{tag}{n}{s}" for n in "bc" for s in "+-"], [f"{tag}C+", f"{tag}C-"], 0.2,
                  lambda c: final(c, rows), sends)

    def rotate(self):
        for r in range(6):
            base, size = BASE[r], SIZE[r]
            piece, half = size // 4, size // 8
            offset = base // 8
            need = [f"{h}{n}{s}" for h in "AB" for s in "+-"
                    for n in (("d0",), ("d1", "f0"), ("d2", "f1"), ("d3", "f2"), ("d4", "f3"), ("f4",))[r]]

            def multiply(c, own, cols, base=base, size=size):
                which = c.k if own else 1 - c.k
                out = c.mine if own else c.other
                if not own and base == 0 and cols == PARTS[0]:
                    c.wait_local("basis")
                where, cols = pl.ds(base, size), pl.ds(*cols)
                out[where, cols] = jnp.dot(c.acts[where, :], c.basis[which, :, cols], preferred_element_type=F32)

            cost = {192: 0.88, 64: 0.62}[size]
            last = f"M{r - 1}m1" if r else "own"
            for own in (False, True):
                for n, cols in enumerate(PARTS):
                    name = f"M{r}{'m' if own else 'o'}{n}"
                    sends = []
                    if not own:
                        sends = [f"{r}core{n}"]
                        self.copy(sends[0], "d", size * cols[1] * 4,
                                  lambda c, base=base, size=size, cols=cols: c.other.at[pl.ds(base, size), pl.ds(*cols)],
                                  lambda c, base=base, size=size, cols=cols: c.partner.at[pl.ds(base, size), pl.ds(*cols)])
                    self.step(name, 70 + 4 * r + 2 * own + n, () if own or n else need, [last], cost,
                              lambda c, f=multiply, own=own, cols=cols: f(c, own, cols), sends)
                    last = name

            def rows(c, d, h, base=base, piece=piece, half=half):
                return ds(base + lax.rem(c.z + d, 4) * piece + h * half, half, 8)

            def recv(c, slot, offset=offset, half=half):
                return c.zland.at[slot, pl.ds(offset, half), :]

            def add(c, where, slot, offset=offset, half=half):
                c.mine[where, :] += c.zland[slot, pl.ds(offset, half), :]

            def begin(c, base=base, size=size):
                c.mine[pl.ds(base, size), :] += c.partner[pl.ds(base, size), :]

            def final(c, rows, base=base, piece=piece, half=half, offset=offset):
                parts = []
                for h, one, two in ((0, 2, 5), (1, 3, 4)):
                    parts.append(c.mine[rows(c, 0, h), :] + c.zland[one, pl.ds(offset, half), :] + c.zland[two, pl.ds(offset, half), :])
                whole = jnp.concatenate(parts, axis=0).astype(BF16)
                where = ds(base + c.z * piece, piece, 16)
                for core in range(2):
                    @pl.when(c.k == core)
                    def _(core=core):
                        c.rot[where, pl.ds(core * HALF, HALF)] = whole

            def place(d, low=0, width=HALF, base=base, piece=piece):
                def ref(c):
                    z = lax.rem(c.z + d, 4)
                    return c.rot.at[ds(base + z * piece, piece, 16), pl.ds(pl.multiple_of(c.k * HALF + low, 128), width)]
                return ref

            rank = 40
            nb = piece * HALF * 2
            self.ring_sum(f"{r}z", "z", rank, half * HALF * 4, rows, lambda c, w: c.mine.at[w, :], recv, add, final,
                          ([f"{r}core0", f"{r}core1"], [f"M{r}m1"], 0.3, begin), [f"{r}g+", f"{r}g-", f"{r}p0"])
            left = 512 if r % 2 else 384
            self.copy(f"{r}g+", "z+", nb, place(0), place(0))
            self.copy(f"{r}g-", "z-", nb, place(0), place(0))
            self.copy(f"{r}h+", "z+", nb * left // HALF, place(3, 0, left), place(3, 0, left))
            self.copy(f"{r}h-", "z-", nb * (HALF - left) // HALF, place(1, left, HALF - left), place(1, left, HALF - left))
            for n, d in (("p0", 0), ("p1", 1), ("p3", 3), ("p2", 2)):
                self.copy(f"{r}{n}", "d", nb, place(d), place(d))
            self.step(f"{r}H+", 38, [f"{r}g+"], sends=[f"{r}h+", f"{r}p3"])
            self.step(f"{r}H-", 38, [f"{r}g-"], sends=[f"{r}h-", f"{r}p1"])
            self.step(f"{r}L", 39, [f"{r}h+", f"{r}h-"], sends=[f"{r}p2"])

            self.step(f"{r}W", 90, [f"{r}p{d}" for d in range(4)], [f"{r}L", f"{r}H+", f"{r}H-"])

    def grads(self):
        nb = 128 * KOUT * 2

        def shard(d, core, low=0, size=128):
            def ref(c):
                k = c.k if core else 1 - c.k
                return c.grads.at[ds((lax.rem(c.z + d, 4) * 2 + k) * 128 + low, size, 16), :]
            return ref

        self.copy("gz+", "z+", nb, shard(0, 1), shard(0, 1))
        self.copy("gz-", "z-", nb, shard(0, 1), shard(0, 1))
        self.copy("gf+", "z+", nb // 2, shard(3, 1, 0, 64), shard(3, 1, 0, 64))
        self.copy("gf-", "z-", nb // 2, shard(1, 1, 64, 64), shard(1, 1, 64, 64))
        for d in range(4):
            self.copy(f"gp{d}", "d", nb, shard(d, 1), shard(d, 1))
        self.step("G0", 1, after=["own"], work=lambda c: c.wait_local("grads"), sends=["gz+", "gz-", "gp0"])
        self.step("GF+", 2, ["gz+"], ["G0"], sends=["gf+", "gp3"])
        self.step("GF-", 2, ["gz-"], ["G0"], sends=["gf-", "gp1"])
        self.step("GL", 2, ["gf+", "gf-"], ["GF+", "GF-"], sends=["gp2"])

        def multiply(c):
            c.wait_local("gbasis")

            @pl.loop(0, 4)
            def _(n):
                where = pl.ds(pl.multiple_of(n * 256, 256), 256)
                part = jnp.dot(c.grads[where, :], c.gbasis[...], preferred_element_type=F32)
                c.gsum[where, :] = part
                c.gsend[where, :] = part.astype(BF16)

        self.step("GM", 3, [f"gp{d}" for d in range(4)], ["GL"], 2.0, multiply)
        for n, (half, one, two) in enumerate((("A", "x", "y"), ("B", "y", "x"), ("C", "x", "y"), ("D", "y", "x"))):
            cols = pl.ds(n * GCOL, GCOL)

            def rows1(c, d, h, one=one):
                return ds(lax.rem(c.pos[one] + d, 4) * 256 + h * 128, 128, 16)

            def add1(c, where, slot, n=n, cols=cols):
                c.gsend[where, cols] = (c.gsum[where, cols] + c.land1[n, slot].astype(F32)).astype(BF16)

            def final1(c, rows, n=n, cols=cols):
                for h, p, q in ((0, 2, 5), (1, 3, 4)):
                    total = c.gsum[rows(c, 0, h), cols] + c.land1[n, p].astype(F32) + c.land1[n, q].astype(F32)
                    c.gsum2[n, pl.ds(h * 128, 128), :] = total
                    c.gsend2[n, pl.ds(h * 128, 128), :] = total.astype(BF16)

            self.ring_sum(f"{half}1", one, 30, 128 * GCOL * 2, rows1, lambda c, w, cols=cols: c.gsend.at[w, cols],
                          lambda c, slot, n=n: c.land1.at[n, slot], add1, final1, ((), ["GM"], 0.05, None), ())

            def rows2(c, d, h, two=two):
                return ds(lax.rem(c.pos[two] + d, 4) * 64 + h * 32, 32, 16)

            def add2(c, where, slot, n=n):
                c.gsend2[n, where, :] = (c.gsum2[n, where, :] + c.land2[n, slot].astype(F32)).astype(BF16)

            def piece(c, d1, d2, one=one, two=two):
                return lax.rem(c.pos[one] + d1, 4) * 256 + lax.rem(c.pos[two] + d2, 4) * 64

            def final2(c, rows, n=n, cols=cols, piece=piece):
                for h, p, q in ((0, 2, 5), (1, 3, 4)):
                    total = c.gsum2[n, rows(c, 0, h), :] + c.land2[n, p].astype(F32) + c.land2[n, q].astype(F32)
                    c.gout[ds(piece(c, 0, 0) + h * 32, 32, 16), cols] = total.astype(BF16)

            def place(d1, d2, low=0, size=64, piece=piece, cols=cols):
                return lambda c: c.gout.at[ds(piece(c, d1, d2) + low, size, 16), cols]

            self.ring_sum(f"{half}2", two, 30, 32 * GCOL * 2, rows2, lambda c, w, n=n: c.gsend2.at[n, w],
                          lambda c, slot, n=n: c.land2.at[n, slot], add2, final2, ((), [f"{half}1E"], 0.05, None),
                          [f"{half}e+", f"{half}e-", f"{half}u0+", f"{half}u0-"])
            nb = 64 * GCOL * 2
            self.copy(f"{half}e+", two + "+", nb, place(0, 0), place(0, 0))
            self.copy(f"{half}e-", two + "-", nb, place(0, 0), place(0, 0))
            self.copy(f"{half}h+", two + "+", nb // 2, place(0, 3, 0, 32), place(0, 3, 0, 32))
            self.copy(f"{half}h-", two + "-", nb // 2, place(0, 1, 32, 32), place(0, 1, 32, 32))
            for j in range(4):
                self.copy(f"{half}u{j}+", one + "+", nb, place(0, j), place(0, j))
                self.copy(f"{half}u{j}-", one + "-", nb, place(0, j), place(0, j))
                self.copy(f"{half}v{j}+", one + "+", nb // 2, place(3, j, 0, 32), place(3, j, 0, 32))
                self.copy(f"{half}v{j}-", one + "-", nb // 2, place(1, j, 32, 32), place(1, j, 32, 32))
                for sign in "+-":
                    self.step(f"{half}V{j}{sign}", 34, [f"{half}u{j}{sign}"], sends=[f"{half}v{j}{sign}"])
            self.step(f"{half}H+", 33, [f"{half}e+"], sends=[f"{half}h+", f"{half}u3+", f"{half}u3-"])
            self.step(f"{half}H-", 33, [f"{half}e-"], sends=[f"{half}h-", f"{half}u1+", f"{half}u1-"])
            self.step(f"{half}L", 33, [f"{half}h+", f"{half}h-"], sends=[f"{half}u2+", f"{half}u2-"])
        every = [f"{h}v{j}{s}" for h in "ABCD" for j in range(4) for s in "+-"]
        self.step("GW", 90, every)


ORDER = (
    26, 99, 13, 1, 14, 101, 0, 23, 100, 27, 10, 28, 29, 15, 2, 3, 30, 102, 16, 31, 39, 103, 123, 40, 104, 41, 17, 42, 43, 24,
    11, 51, 32, 18, 5, 52, 106, 4, 33, 105, 53, 54, 45, 125, 44, 55, 12, 124, 161, 142, 25, 46, 63, 34, 57, 56, 64, 7, 65,
    20, 126, 66, 19, 67, 6, 143, 162, 163, 127, 144, 9, 48, 21, 47, 107, 22, 58, 108, 36, 68, 8, 35, 69, 75, 76, 164, 165,
    128, 145, 146, 129, 77, 78, 79, 110, 109, 87, 166, 167, 88, 148, 147, 130, 89, 90, 91, 111, 168, 80, 81, 149, 139, 140,
    70, 93, 120, 121, 177, 178, 92, 158, 159, 82, 169, 122, 170, 141, 137, 94, 179, 160, 71, 60, 115, 172, 59, 132, 153, 138,
    118, 175, 150, 72, 119, 37, 112, 131, 114, 116, 117, 84, 83, 151, 133, 49, 152, 136, 176, 171, 157, 134, 113, 156, 135,
    95, 96, 173, 174, 154, 155, 61, 50, 73, 38, 85, 74, 97, 62, 86, 180, 98,
)


class Context:
    pass


def rotate_kernel(plan, acts_in, basis_in, grads_in, gbasis_in, rot, gout,
                  acts, basis, mine, other, partner, zland, grads, gbasis, gsum, gsend, gsum2, gsend2, land1, land2,
                  send_sem, recv_sem, load_sem):
    c = Context()
    c.acts, c.basis, c.mine, c.other, c.partner, c.zland, c.rot = acts, basis, mine, other, partner, zland, rot
    c.grads, c.gbasis, c.gsum, c.gsend, c.gsum2, c.gsend2 = grads, gbasis, gsum, gsend, gsum2, gsend2
    c.land1, c.land2, c.gout = land1, land2, gout
    row, col = lax.axis_index("row"), lax.axis_index("col")
    c.pos = {"x": row // 4, "y": lax.rem(row, 4)}
    c.z, c.k = col // 2, lax.rem(col, 2)

    def peer(link):
        if link == "d":
            return (row, c.z * 2 + 1 - c.k)
        step = 1 if link[1] == "+" else 3
        if link[0] == "z":
            return (row, lax.rem(c.z + step, 4) * 2 + c.k)
        if link[0] == "x":
            return (lax.rem(c.pos["x"] + step, 4) * 4 + c.pos["y"], col)
        return (c.pos["x"] * 4 + lax.rem(c.pos["y"] + step, 4), col)

    me = col * 128
    loads = {
        "acts": [(acts_in.at[pl.ds(0, 32), :], acts.at[pl.ds(ROW["A00"], 32), :]),
                 (acts_in.at[pl.ds(32, 32), :], acts.at[pl.ds(ROW["B00"], 32), :])],
        "grads": [(grads_in, grads.at[ds(me, 128, 128), :])],
        "gbasis": [(gbasis_in, gbasis)],
        "basis": [(basis_in.at[pl.ds(q * 896, 896), pl.ds(h * HALF, HALF)], basis.at[h, pl.ds(q * 896, 896), :])
                  for q in range(4) for h in range(2)],
    }
    number, local = 0, {}
    for name, pairs in loads.items():
        local[name] = []
        for src, dst in pairs:
            local[name].append(pltpu.make_async_copy(src, dst, load_sem.at[number]))
            number += 1
            local[name][-1].start()

    def wait_local(name):
        for one in local[name]:
            one.wait()

    c.wait_local = wait_local
    barrier = pltpu.get_barrier_semaphore()
    links = ("x+", "x-", "y+", "y-", "z+", "z-", "d")
    for link in links:
        pl.semaphore_signal(barrier, inc=1, device_id=peer(link), device_id_type=MESH)
    pl.semaphore_wait(barrier, len(links))

    started = {}

    def copy_of(name):
        link, _, src, dst = plan.copies[name]
        n = plan.index[name]
        return pltpu.make_async_remote_copy(src_ref=src(c), dst_ref=dst(c), send_sem=send_sem.at[n], recv_sem=recv_sem.at[n],
                                            device_id=peer(link), device_id_type=MESH)

    waited = set()
    names = list(plan.steps)
    for name in (names[n] for n in ORDER):
        _, waits, _, _, work, sends = plan.steps[name]
        for one in waits:
            if one not in waited:
                waited.add(one)
                started[one].wait_recv()
        if work is not None:
            work(c)
        for one in sends:
            started[one] = copy_of(one)
            started[one].start()
    assert waited == set(plan.copies)
    for one in started.values():
        one.wait_send()


def rotate(activations, act_basis, grads, grad_basis):
    plan = Plan()
    count = len(plan.copies)
    anywhere = pl.BlockSpec(memory_space=pl.ANY)
    return pl.pallas_call(
        lambda *refs: rotate_kernel(plan, *refs),
        out_shape=[pltpu.VMEM((TOKENS, NIN), BF16), pltpu.VMEM((TOKENS, NOUT), BF16)],
        in_specs=[anywhere] * 4,
        out_specs=[pl.BlockSpec(memory_space=pltpu.VMEM)] * 2,
        scratch_shapes=[
            pltpu.VMEM((TOKENS, KIN), BF16),
            pltpu.VMEM((2, KIN, HALF), BF16),
            pltpu.VMEM((TOKENS, HALF), F32),
            pltpu.VMEM((TOKENS, HALF), F32),
            pltpu.VMEM((TOKENS, HALF), F32),
            pltpu.VMEM((6, TOKENS // 8, HALF), F32),
            pltpu.VMEM((TOKENS, KOUT), BF16),
            pltpu.VMEM((KOUT, NOUT), BF16),
            pltpu.VMEM((TOKENS, NOUT), F32),
            pltpu.VMEM((TOKENS, NOUT), BF16),
            pltpu.VMEM((4, 256, GCOL), F32),
            pltpu.VMEM((4, 256, GCOL), BF16),
            pltpu.VMEM((4, 6, 128, GCOL), BF16),
            pltpu.VMEM((4, 6, 32, GCOL), BF16),
            pltpu.SemaphoreType.DMA((count,)),
            pltpu.SemaphoreType.DMA((count,)),
            pltpu.SemaphoreType.DMA((12,)),
        ],
        compiler_params=pltpu.CompilerParams(collective_id=0, has_side_effects=True, vmem_limit_bytes=50 * 2**20),
        name="rotate",
    )(activations, act_basis, grads, grad_basis)


def square_kernel(rot, grad, out, held, sem):
    row = lax.axis_index("row")
    x, y = row // 4, lax.rem(row, 4)
    order = [[(half, i, j) for half in "AB" for j in range(4)] for i in range(4)]

    def token(h, i, j):
        return (lax.rem(x + i, 4) * 4 + lax.rem(y + j, 4)) * 64 + (0 if h == "A" else 32)

    tile, copies = 256, []
    for r in range(0, NIN, tile):
        left = [jnp.concatenate([rot[pl.ds(ROW[f"{h}{i}{j}"], 32), r : r + tile] for h, i, j in blocks], axis=0) for blocks in order]
        for n in range(0, NOUT, tile):
            total = None
            for s, blocks in enumerate(order):
                right = jnp.concatenate([grad[ds(token(h, i, j), 32, 32), n : n + tile] for h, i, j in blocks], axis=0)
                products = lax.dot_general(left[s], right, (((0,), (0,)), ((), ())), preferred_element_type=F32)
                total = products * products if total is None else total + products * products
            held[r : r + tile, n : n + tile] = total * (1.0 / (LEN * SEQS))
            where = (pl.ds(r, tile), pl.ds(n, tile))
            copies.append(pltpu.make_async_copy(held.at[where], out.at[where], sem.at[len(copies)]))
            copies[-1].start()
    for one in copies:
        one.wait()


def square(rot, grad):
    return pl.pallas_call(
        square_kernel,
        out_shape=jax.ShapeDtypeStruct((NIN, NOUT), F32),
        in_specs=[pl.BlockSpec(memory_space=pltpu.VMEM)] * 2,
        out_specs=pl.BlockSpec(memory_space=pl.ANY),
        scratch_shapes=[pltpu.VMEM((NIN, NOUT), F32), pltpu.SemaphoreType.DMA((28,))],
        compiler_params=pltpu.CompilerParams(vmem_limit_bytes=20 * 2**20),
        name="square",
    )(rot, grad)


def shards(activations, act_basis, grads, grad_basis):
    return square(*rotate(activations, act_basis, grads, grad_basis))


def solution(mesh):
    return jax.shard_map(
        shards,
        mesh=mesh,
        in_specs=(P("row", "col"), P("col", "row"), P("col", "row"), P("row", "col")),
        out_specs=P("row", "col"),
        check_vma=False,
    )
```
